32 devices in a mesh: lat: 8 (over y, x, core), lon: 4 (over z).
Axes of the slice: x: 2, y: 2, z: 4, core: 2. Of those that a mesh axis runs over, the one named last changes fastest.
Arguments:
- fields: float32 [4, 6, 256, 1280], P(None, None, 'lat', 'lon'), may hold values from -6 to 6
- dep_row: int32 [6, 256, 1280], P(None, 'lat', 'lon'), may hold values from -4 to 255, as said below
- dep_col: int32 [6, 256, 1280], P(None, 'lat', 'lon'), may hold values from 0 to 1279, as said below
- weights: float32 [8, 6, 256, 1280], P(None, None, 'lat', 'lon'), may hold values from -0.25 to 0.75
Outputs:
- departed: float32 [4, 6, 256, 1280], P(None, None, 'lat', 'lon')
The draws below stay inside these ranges and needn't reach their ends.
Inputs may be any that keep to these rules, and one draw needn't show every extreme that they name: dep_row[l, i, j] lies within i - 4 to i. dep_col[l, i, j] equals (j + k) modulo 1280 for some k from -4 to 0.
All inputs are finite; a program needn't handle non-finite values.
Results may differ from the reference program's by a relative error of at most 0.0003.
Values sent between devices are 32-bit elements; how exact they have to be, the bound alone decides.
No kernel may reach another device: no remote copies, remote signals or barrier semaphores. Data moves between devices by JAX's collectives and lax.ppermute only.
A program may use at most 64 MiB of HBM per device.

```python
import jax
import jax.numpy as jnp
from jax import lax

LEV = 6
FIELDS = 4
HALO = 4
NR = 256
NC = 1280


def departures(key):
    base_key = jax.random.fold_in(key, 7713)
    key_rows, key_cols = jax.random.split(base_key)
    shape = (LEV, NR, NC)
    shift_rows = jax.random.randint(key_rows, shape, -3, 2, dtype=jnp.int32)
    shift_cols = jax.random.randint(key_cols, shape, -3, 2, dtype=jnp.int32)
    row_index = lax_iota(shape, 1)
    col_index = lax_iota(shape, 2)
    rows = row_index + shift_rows - 1
    cols = jnp.mod(col_index + shift_cols - 1, NC)
    return (rows.astype(jnp.int32), cols.astype(jnp.int32))


def lax_iota(shape, dim):
    return jax.lax.broadcasted_iota(jnp.int32, shape, dim)


def draw_dep_row(key, part):
    return departures(key)[0]


def draw_dep_col(key, part):
    return departures(key)[1]


def block_levels(stream_key, dims, cuts, least, top_value):
    gain, own = 1.0, jax.random.fold_in(stream_key, 6)
    for dim, blocks in cuts:
        steps = jnp.exp(jax.random.uniform(jax.random.fold_in(own, dim), (blocks,), jnp.float32, least / len(cuts), top_value / len(cuts)))
        gain = gain * jnp.repeat(steps, dims[dim] // blocks).reshape([-1 if axis == dim else 1 for axis in range(len(dims))])
    return gain


def bell_draw(own_key, extent, deviation, most, pieces=(), held_as=jnp.bfloat16):
    drawn = deviation * jax.random.normal(own_key, extent, jnp.float32)
    if pieces:
        drawn = drawn * block_levels(own_key, extent, pieces, -0.22, 0.18)
    return jnp.clip(drawn, -most, most).astype(held_as)


def setup_inputs(seed: int = 0) -> dict:
    key_of = jax.random.split(jax.random.key(seed), 5)
    return {
        "fields": bell_draw(key_of[0], (FIELDS, LEV, NR, NC), 1.0, 6.0, ((2, 8), (3, 4)), jnp.float32),
        "dep_row": draw_dep_row(jax.random.fold_in(key_of[4], 71), 0),
        "dep_col": draw_dep_col(jax.random.fold_in(key_of[4], 71), 0),
        "weights": jnp.clip(-0.25 + 1.0 * jax.random.uniform(key_of[3], (8, LEV, NR, NC), jnp.float32) ** block_levels(key_of[3], (8, LEV, NR, NC), ((2, 8), (3, 4)), -0.2, 0.2), -0.25, 0.75),
    }


def interpolate_level(item):
    field, rows, cols, weight = item
    half = NC // 2
    north = jnp.roll(field[:, :HALO][:, ::-1], half, axis=2)
    south = jnp.roll(field[:, NR - HALO:][:, ::-1], half, axis=2)
    tall = jnp.concatenate([north, field, south], axis=1)
    padded = jnp.concatenate([tall[:, :, NC - HALO:], tall, tall[:, :, :HALO]], axis=2)
    width = NC + 2 * HALO
    flat = padded.reshape(FIELDS, -1)
    base = ((rows + HALO) * width + (cols + HALO)).astype(jnp.int32).reshape(-1)
    total = jnp.zeros((FIELDS, NR * NC), jnp.float32)
    for first in range(4):
        line = jnp.zeros((FIELDS, NR * NC), jnp.float32)
        for second in range(4):
            values = jnp.take(flat, base + first * width + second, axis=1)
            line = line + weight[4 + second].reshape(1, -1) * values
        total = total + weight[first].reshape(1, -1) * line
    return total.reshape(FIELDS, NR, NC)


def reference(fields, dep_row, dep_col, weights):
    result = lax.map(interpolate_level, (jnp.transpose(fields, (1, 0, 2, 3)), dep_row, dep_col, jnp.transpose(weights, (1, 0, 2, 3))))
    return jnp.transpose(result, (1, 0, 2, 3))
```

```python
import jax
import jax.numpy as jnp
from jax import lax
from jax.experimental import pallas as pl
from jax.experimental.pallas import tpu as pltpu
from jax.sharding import PartitionSpec as P

HALO = 4
TAPS = 2 * HALO
LANES = 128
SUB = 8
VMEM = 48 * 1024 * 1024


def iota(dim):
    return lax.broadcasted_iota(jnp.int32, (SUB, LANES), dim)


def expand(k, w):
    masks = [k == v for v in range(HALO + 1)]
    out = []
    for t in range(TAPS):
        val = jnp.zeros((SUB, LANES), jnp.float32)
        for v in range(HALO + 1):
            if 0 <= t - v < 4:
                val = jnp.where(masks[v], w[t - v], val)
        out.append(val)
    return out


def shifted(prev, cur, nxt, t):
    lane = iota(1)
    if t < HALO:
        d = HALO - t
        return pltpu.roll(jnp.where(lane >= LANES - d, prev, cur), d, 1)
    if t == HALO:
        return cur
    e = t - HALO
    z = cur if nxt is None else jnp.where(lane < e, nxt, cur)
    return pltpu.roll(z, LANES - e, 1)


def col_first(dep, base, total_cols):
    off = dep - base - iota(1)
    return jnp.where(off > 0, off - total_cols, off) + HALO


def pack_kernel(first_ref, last_ref, west_ref, east_ref, *, rem, tiles):
    lane = iota(1)
    nf, nl = first_ref.shape[:2]
    for l in range(nl):
        w = jnp.zeros((SUB, LANES), jnp.float32)
        e = jnp.zeros((SUB, LANES), jnp.float32)
        for f in range(nf):
            for rt in range(tiles):
                m = HALO * (f * tiles + rt)
                here = (lane >= m) & (lane < m + HALO)
                a = last_ref[f, l, rt * SUB : rt * SUB + SUB, :]
                b = first_ref[f, l, rt * SUB : rt * SUB + SUB, :]
                w = jnp.where(here, pltpu.roll(a, (m - (rem - HALO)) % LANES, 1), w)
                e = jnp.where(here, pltpu.roll(b, m, 1), e)
        west_ref[l] = w
        east_ref[l] = e


def halo_tiles(west, east, slot, last, rem):
    m = HALO * slot
    prev = pltpu.roll(west, (LANES - HALO - m) % LANES, 1)
    ends = jnp.where(iota(1) < rem, last, pltpu.roll(east, (rem - m) % LANES, 1))
    return prev, ends


def rowpack_kernel(top_ref, bot_ref, west_ref, east_ref, cw_ref, ccw_ref, *, rem, tiles, n, half):
    nf, nl = top_ref.shape[:2]
    band = lax.axis_index("lat")
    sector = lax.axis_index("lon")
    last_band = lax.axis_size("lat") - 1
    sub = iota(0)
    upper = sub < HALO
    full = lambda x: jnp.full((SUB, LANES), x, jnp.int32)
    flip = jnp.where(upper, full(band), last_band - full(band)) == 0
    low = full(sector) < half

    def cut(ref, f, l, q):
        return ref[f, l, :, q * LANES : (q + 1) * LANES] if q < n - 1 else ref[f, l, :, q * LANES :]

    for l in range(nl):
        west, east = west_ref[l], east_ref[l]
        for f in range(nf):
            t = []
            for q in range(n):
                a = top_ref[f, l, :, q * LANES : (q + 1) * LANES]
                b = bot_ref[f, l, :, q * LANES : (q + 1) * LANES]
                t.append(jnp.where(upper, a, b))
            slot_t, slot_b = f * tiles, f * tiles + tiles - 1
            pa, ea = halo_tiles(west, east, slot_t, t[-1], rem)
            pb, eb = halo_tiles(west, east, slot_b, t[-1], rem)
            prev = jnp.where(upper, pa, pb)
            t[-1] = jnp.where(upper, ea, eb)
            for q in range(n):
                v = shifted(t[q - 1] if q else prev, t[q], None, 0)
                r1 = sub % HALO
                rev = jnp.where(
                    r1 == 0,
                    pltpu.roll(v, SUB - 3, 0),
                    jnp.where(
                        r1 == 1,
                        pltpu.roll(v, SUB - 1, 0),
                        jnp.where(r1 == 2, pltpu.roll(v, 1, 0), pltpu.roll(v, 3, 0)),
                    ),
                )
                v = jnp.where(flip, rev, v)
                s = pltpu.roll(v, HALO, 0)
                cw_ref[f, l, :, q * LANES : (q + 1) * LANES] = jnp.where(low, s, v)[:HALO]
                ccw_ref[f, l, :, q * LANES : (q + 1) * LANES] = jnp.where(low, v, s)[:HALO]


def tile_loop(s_ref, base, rt, kr, kc, w, nf, emit):
    r = expand(kr, w[:4])
    c = expand(kc, w[4:])
    for f in range(nf):
        total = None
        for s in range(TAPS):
            line = None
            for t in range(TAPS):
                term = c[t] * s_ref[base(f), t, pl.ds(rt * SUB + HALO + s, SUB), :]
                line = term if line is None else line + term
            line = r[s] * line
            total = line if total is None else total + line
        emit(f, total)


def clear_margins(s_ref, rows):
    zero = jnp.zeros((SUB, LANES), jnp.float32)
    for i in range(s_ref.shape[0]):
        for t in range(TAPS):
            s_ref[i, t, 0:SUB, :] = zero
            s_ref[i, t, SUB + rows : 2 * SUB + rows, :] = zero


def inner_kernel(x_ref, row_ref, col_ref, w_ref, o_ref, s_ref, *, rows, cols, total_cols):
    nf = x_ref.shape[0]
    tiles = rows // SUB
    row0 = lax.axis_index("lat") * rows
    col0 = lax.axis_index("lon") * cols + LANES

    @pl.when(pl.program_id(0) == 0)
    def _():
        clear_margins(s_ref, rows)

    for f in range(nf):
        for rt in range(tiles):
            x = [x_ref[f, 0, rt * SUB : rt * SUB + SUB, q * LANES : (q + 1) * LANES] for q in (0, 1, 2)]
            for t in range(TAPS):
                s_ref[f, t, SUB + rt * SUB : 2 * SUB + rt * SUB, :] = shifted(x[0], x[1], x[2], t)

    def step(rt, carry):
        at = pl.ds(pl.multiple_of(rt * SUB, SUB), SUB)
        kr = row_ref[0, at, :] - (row0 + rt * SUB - HALO) - iota(0)
        kc = col_first(col_ref[0, at, :], col0, total_cols)
        w = [w_ref[b, 0, at, :] for b in range(8)]

        def emit(f, v):
            o_ref[f, 0, at, :] = v

        tile_loop(s_ref, lambda f: f, rt, kr, kc, w, nf, emit)
        return carry

    lax.fori_loop(0, tiles, step, 0)


def outer_kernel(
    x_ref, row_ref, col_ref, w_ref, west_ref, east_ref, mid_ref, o_ref, s_ref, *, rows, cols, rem, n, total_cols
):
    nf = x_ref.shape[0]
    tiles = rows // SUB
    row0 = lax.axis_index("lat") * rows
    col0 = lax.axis_index("lon") * cols

    @pl.when(pl.program_id(0) == 0)
    def _():
        clear_margins(s_ref, rows)

    west, east = west_ref[0], east_ref[0]
    for f in range(nf):
        for rt in range(tiles):
            x = [x_ref[f, 0, rt * SUB : rt * SUB + SUB, q * LANES : (q + 1) * LANES] for q in range(n)]
            prev, x[-1] = halo_tiles(west, east, f * tiles + rt, x[-1], rem)
            to = slice(SUB + rt * SUB, 2 * SUB + rt * SUB)
            for t in range(TAPS):
                s_ref[f, t, to, :] = shifted(prev, x[0], x[1], t)
                s_ref[nf + f, t, to, :] = shifted(x[-2], x[-1], None, t)

    for f in range(nf):
        o_ref[f, 0, :, LANES : 2 * LANES] = mid_ref[f, 0]

    def step(rt, carry):
        at = pl.ds(pl.multiple_of(rt * SUB, SUB), SUB)
        for side, q in enumerate((0, n - 1)):
            lanes = slice(q * LANES, (q + 1) * LANES)
            kr = row_ref[0, at, lanes] - (row0 + rt * SUB - HALO) - iota(0)
            kc = col_first(col_ref[0, at, lanes], col0 + q * LANES, total_cols)
            w = [w_ref[b, 0, at, lanes] for b in range(8)]

            def emit(f, v):
                o_ref[f, 0, at, lanes] = v

            tile_loop(s_ref, lambda f: side * nf + f, rt, kr, kc, w, nf, emit)
        return carry

    lax.fori_loop(0, tiles, step, 0)


def edge_kernel(
    cw_ref, ccw_ref, rt_ref, rb_ref, ct_ref, cb_ref, wt_ref, wb_ref, o_in, o_out, top, bot, sems,
    *, rows, cols, n, half, total_cols
):
    nf, nl = cw_ref.shape[:2]
    ins = [
        pltpu.make_async_copy(o_in.at[:, :, pl.ds(0, SUB), :], top, sems.at[0]),
        pltpu.make_async_copy(o_in.at[:, :, pl.ds(rows - SUB, SUB), :], bot, sems.at[1]),
    ]
    for c in ins:
        c.start()
    for c in ins:
        c.wait()
    row0 = lax.axis_index("lat") * rows
    col0 = lax.axis_index("lon") * cols
    upper = iota(0) < HALO
    low = jnp.full((SUB, LANES), lax.axis_index("lon"), jnp.int32) < half
    lane, sub = iota(1), iota(0)
    zero = jnp.zeros((SUB, LANES), jnp.float32)
    pad = jnp.zeros((SUB - HALO, LANES), jnp.float32)

    def level(l, carry):
        rc = []
        for q in range(n):
            lanes = slice(q * LANES, (q + 1) * LANES)
            pick = lambda a, b: jnp.where(upper, a, b)
            first = pick(sub + row0, sub + (row0 + rows - SUB))
            kr = pick(rt_ref[l, :, lanes], rb_ref[l, :, lanes]) - first + HALO
            kc = col_first(pick(ct_ref[l, :, lanes], cb_ref[l, :, lanes]), col0 + q * LANES, total_cols)
            w = [pick(wt_ref[b, l, :, lanes], wb_ref[b, l, :, lanes]) for b in range(8)]
            r = expand(kr, w[:4])
            rc.append(([pick(r[s], r[s + HALO]) for s in range(HALO)], expand(kc, w[4:])))
        for f in range(nf):
            v = []
            for q in range(n):
                lanes = slice(q * LANES, (q + 1) * LANES)
                a = jnp.concatenate([cw_ref[f, l, :, lanes], pad], axis=0)
                b = jnp.concatenate([ccw_ref[f, l, :, lanes], pad], axis=0)
                a, b = jnp.where(low, a, b), jnp.where(low, b, a)
                v.append([a] + [pltpu.roll(jnp.where(sub < s, b, a), SUB - s, 0) for s in range(1, HALO)])
            v.append([zero] * HALO)
            for q in range(n):
                r, c = rc[q]
                total = None
                for s in range(HALO):
                    line = None
                    for t in range(TAPS):
                        x = v[q][s]
                        if t:
                            x = pltpu.roll(jnp.where(lane < t, v[q + 1][s], x), LANES - t, 1)
                        line = c[t] * x if line is None else line + c[t] * x
                    line = r[s] * line
                    total = line if total is None else total + line
                lanes = slice(q * LANES, min((q + 1) * LANES, cols))
                total = total[:, : min(LANES, cols - q * LANES)]
                keep = upper[:, : total.shape[1]]
                top[f, l, :, lanes] += jnp.where(keep, total, 0.0)
                bot[f, l, :, lanes] += jnp.where(keep, 0.0, total)
        return carry

    lax.fori_loop(0, nl, level, 0)
    outs = [
        pltpu.make_async_copy(top, o_out.at[:, :, pl.ds(0, SUB), :], sems.at[0]),
        pltpu.make_async_copy(bot, o_out.at[:, :, pl.ds(rows - SUB, SUB), :], sems.at[1]),
    ]
    for c in outs:
        c.start()
    for c in outs:
        c.wait()


def circle(lat, lon):
    half = lon // 2
    pairs = []
    for s in range(lon):
        for b in range(lat):
            step = 1 if s < half else -1
            to = (b + step, s) if 0 <= b + step < lat else (b, (s + half) % lon)
            pairs.append((b * lon + s, to[0] * lon + to[1]))
    return pairs


def body(fields, dep_row, dep_col, weights):
    nf, nl, rows, cols = fields.shape
    lat, lon = lax.axis_size("lat"), lax.axis_size("lon")
    n = -(-cols // LANES)
    rem = cols - (n - 1) * LANES
    tiles = rows // SUB
    wide = n * LANES
    half = lon // 2
    total_cols = cols * lon
    assert n == 3 and HALO <= rem <= LANES - HALO and rows % SUB == 0
    f32 = jnp.float32
    shape = jax.ShapeDtypeStruct
    params = lambda: pltpu.CompilerParams(vmem_limit_bytes=VMEM)
    strip = shape((nl, SUB, LANES), f32)
    i0 = lambda *_: (0, 0, 0)

    def lane_block(q):
        return pl.BlockSpec((nf, nl, rows, LANES), lambda i: (0, 0, 0, q))

    west_out, east_out = pl.pallas_call(
        lambda *a: pack_kernel(*a, rem=rem, tiles=tiles),
        grid=(1,),
        in_specs=[lane_block(0), lane_block(n - 1)],
        out_specs=[pl.BlockSpec(strip.shape, i0)] * 2,
        out_shape=[strip, strip],
        compiler_params=params(),
        name="pack",
    )(fields, fields)
    up = [(i, (i + 1) % lon) for i in range(lon)]
    west = lax.ppermute(west_out, "lon", up)
    east = lax.ppermute(east_out, "lon", [(j, i) for i, j in up])

    level4 = lambda k, w: pl.BlockSpec((k, 1, rows, w), lambda l: (0, l, 0, 0))
    level3 = pl.BlockSpec((1, rows, wide), lambda l: (l, 0, 0))
    mid4 = lambda k: pl.BlockSpec((k, 1, rows, LANES), lambda l: (0, l, 0, 1))
    mid3 = pl.BlockSpec((1, rows, LANES), lambda l: (l, 0, 1))
    mid = pl.pallas_call(
        lambda *a: inner_kernel(*a, rows=rows, cols=cols, total_cols=total_cols),
        grid=(nl,),
        in_specs=[level4(nf, wide), mid3, mid3, mid4(8)],
        out_specs=pl.BlockSpec((nf, 1, rows, LANES), lambda l: (0, l, 0, 0)),
        out_shape=shape((nf, nl, rows, LANES), f32),
        scratch_shapes=[pltpu.VMEM((nf, TAPS, rows + 2 * SUB, LANES), f32)],
        compiler_params=params(),
        name="inner",
    )(fields, dep_row, dep_col, weights)

    edge4 = lambda k, r: pl.BlockSpec((k, nl, SUB, wide), lambda i: (0, 0, r, 0))
    edge3 = lambda r: pl.BlockSpec((nl, SUB, wide), lambda i: (0, r, 0))
    band_edge = shape((nf, nl, HALO, wide), f32)
    whole4 = pl.BlockSpec(band_edge.shape, lambda i: (0, 0, 0, 0))
    whole3 = pl.BlockSpec(strip.shape, i0)
    cw, ccw = pl.pallas_call(
        lambda *a: rowpack_kernel(*a, rem=rem, tiles=tiles, n=n, half=half),
        grid=(1,),
        in_specs=[edge4(nf, 0), edge4(nf, tiles - 1), whole3, whole3],
        out_specs=[whole4] * 2,
        out_shape=[band_edge] * 2,
        compiler_params=params(),
        name="rowpack",
    )(fields, fields, west, east)
    ring = circle(lat, lon)
    cw = lax.ppermute(cw, ("lat", "lon"), ring)
    ccw = lax.ppermute(ccw, ("lat", "lon"), [(j, i) for i, j in ring])

    strip_l = pl.BlockSpec((1, SUB, LANES), lambda l: (l, 0, 0))
    out = pl.pallas_call(
        lambda *a: outer_kernel(*a, rows=rows, cols=cols, rem=rem, n=n, total_cols=total_cols),
        grid=(nl,),
        in_specs=[level4(nf, wide), level3, level3, level4(8, wide), strip_l, strip_l,
                  pl.BlockSpec((nf, 1, rows, LANES), lambda l: (0, l, 0, 0))],
        out_specs=level4(nf, wide),
        out_shape=shape(fields.shape, f32),
        scratch_shapes=[pltpu.VMEM((2 * nf, TAPS, rows + 2 * SUB, LANES), f32)],
        compiler_params=params(),
        name="outer",
    )(fields, dep_row, dep_col, weights, west, east, mid)

    hbm = pl.BlockSpec(memory_space=pl.ANY)
    return pl.pallas_call(
        lambda *a: edge_kernel(*a, rows=rows, cols=cols, n=n, half=half, total_cols=total_cols),
        grid=(1,),
        in_specs=[whole4, whole4, edge3(0), edge3(tiles - 1), edge3(0), edge3(tiles - 1),
                  edge4(8, 0), edge4(8, tiles - 1), hbm],
        out_specs=hbm,
        out_shape=shape(fields.shape, f32),
        scratch_shapes=[pltpu.VMEM((nf, nl, SUB, cols), f32), pltpu.VMEM((nf, nl, SUB, cols), f32),
                        pltpu.SemaphoreType.DMA((2,))],
        input_output_aliases={8: 0},
        compiler_params=params(),
        name="edge",
    )(cw, ccw, dep_row, dep_row, dep_col, dep_col, weights, weights, out)


def solution(mesh):
    return jax.shard_map(
        body,
        mesh=mesh,
        in_specs=(
            P(None, None, "lat", "lon"),
            P(None, "lat", "lon"),
            P(None, "lat", "lon"),
            P(None, None, "lat", "lon"),
        ),
        out_specs=P(None, None, "lat", "lon"),
        check_vma=False,
    )
```

```python
import jax
import jax.numpy as jnp
from jax import lax
from jax.experimental import pallas as pl
from jax.experimental.pallas import tpu as pltpu
from jax.sharding import PartitionSpec as P

HALO = 4
TAPS = 2 * HALO
LANES = 128
SUB = 8
VMEM = 24 * 1024 * 1024


def iota(dim):
    return lax.broadcasted_iota(jnp.int32, (SUB, LANES), dim)


def tile(ref, lead, row, q, n, rem):
    at = pl.ds(row, SUB)
    if q < n - 1 or rem == LANES:
        return ref[(*lead, at, slice(q * LANES, (q + 1) * LANES))]
    part = ref[(*lead, at, slice(q * LANES, q * LANES + rem))]
    fill = jnp.zeros((SUB, LANES - rem), part.dtype)
    return jnp.concatenate([part, fill], axis=1)


def expand(k, w):
    masks = [k == v for v in range(HALO + 1)]
    out = []
    for t in range(TAPS):
        val = jnp.zeros((SUB, LANES), jnp.float32)
        for v in range(HALO + 1):
            if 0 <= t - v < 4:
                val = jnp.where(masks[v], w[t - v], val)
        out.append(val)
    return out


def shifted(prev, cur, nxt, t):
    lane = iota(1)
    if t < HALO:
        d = HALO - t
        return pltpu.roll(jnp.where(lane >= LANES - d, prev, cur), d, 1)
    if t == HALO:
        return cur
    e = t - HALO
    z = cur if nxt is None else jnp.where(lane < e, nxt, cur)
    return pltpu.roll(z, LANES - e, 1)


def col_first(dep, base, total_cols):
    off = dep - base - iota(1)
    return jnp.where(off > 0, off - total_cols, off) + HALO


def pack_kernel(x_ref, west_ref, east_ref, *, rem, tiles, n):
    lane = iota(1)
    nf, nl = x_ref.shape[:2]
    for l in range(nl):
        w = jnp.zeros((SUB, LANES), jnp.float32)
        e = jnp.zeros((SUB, LANES), jnp.float32)
        for f in range(nf):
            for rt in range(tiles):
                m = HALO * (f * tiles + rt)
                here = (lane >= m) & (lane < m + HALO)
                a = tile(x_ref, (f, l), rt * SUB, n - 1, n, rem)
                b = tile(x_ref, (f, l), rt * SUB, 0, n, rem)
                w = jnp.where(here, pltpu.roll(a, (m - (rem - HALO)) % LANES, 1), w)
                e = jnp.where(here, pltpu.roll(b, m, 1), e)
        west_ref[l] = w
        east_ref[l] = e


def halo_tiles(west, east, slot, last, rem):
    m = HALO * slot
    prev = pltpu.roll(west, (LANES - HALO - m) % LANES, 1)
    ends = jnp.where(iota(1) < rem, last, pltpu.roll(east, (rem - m) % LANES, 1))
    return prev, ends


def rowpack_kernel(x_ref, west_ref, east_ref, after, cw_ref, ccw_ref, *, rem, tiles, n, half):
    nf, nl, rows, _ = x_ref.shape
    band = lax.axis_index("lat")
    sector = lax.axis_index("lon")
    last_band = lax.axis_size("lat") - 1
    sub = iota(0)
    upper = sub < HALO
    full = lambda x: jnp.full((SUB, LANES), x, jnp.int32)
    flip = jnp.where(upper, full(band), last_band - full(band)) == 0
    low = full(sector) < half

    for l in range(nl):
        west, east = west_ref[l], east_ref[l]
        for f in range(nf):
            t = []
            for q in range(n):
                a = tile(x_ref, (f, l), 0, q, n, rem)
                b = tile(x_ref, (f, l), rows - SUB, q, n, rem)
                t.append(jnp.where(upper, a, b))
            slot_t, slot_b = f * tiles, f * tiles + tiles - 1
            pa, ea = halo_tiles(west, east, slot_t, t[-1], rem)
            pb, eb = halo_tiles(west, east, slot_b, t[-1], rem)
            prev = jnp.where(upper, pa, pb)
            t[-1] = jnp.where(upper, ea, eb)
            for q in range(n):
                v = shifted(t[q - 1] if q else prev, t[q], None, 0)
                r1 = sub % HALO
                rev = jnp.where(
                    r1 == 0,
                    pltpu.roll(v, SUB - 3, 0),
                    jnp.where(
                        r1 == 1,
                        pltpu.roll(v, SUB - 1, 0),
                        jnp.where(r1 == 2, pltpu.roll(v, 1, 0), pltpu.roll(v, 3, 0)),
                    ),
                )
                v = jnp.where(flip, rev, v)
                s = pltpu.roll(v, HALO, 0)
                cw_ref[f, l, :, q * LANES : (q + 1) * LANES] = jnp.where(low, s, v)[:HALO]
                ccw_ref[f, l, :, q * LANES : (q + 1) * LANES] = jnp.where(low, v, s)[:HALO]


def tile_loop(s_ref, base, rt, kr, kc, w, nf, emit):
    r = expand(kr, w[:4])
    c = expand(kc, w[4:])
    for f in range(nf):
        total = None
        for s in range(TAPS):
            line = None
            for t in range(TAPS):
                term = c[t] * s_ref[base(f), t, pl.ds(rt * SUB + HALO + s, SUB), :]
                line = term if line is None else line + term
            line = r[s] * line
            total = line if total is None else total + line
        emit(f, total)


def clear_margins(s_ref, rows):
    zero = jnp.zeros((SUB, LANES), jnp.float32)
    for i in range(s_ref.shape[0]):
        for t in range(TAPS):
            s_ref[i, t, 0:SUB, :] = zero
            s_ref[i, t, SUB + rows : 2 * SUB + rows, :] = zero


def inner_kernel(x_ref, row_ref, col_ref, w_ref, o_ref, s_ref, *, rows, cols, rem, n, total_cols):
    nf, nl = x_ref.shape[:2]
    tiles = rows // SUB
    row0 = lax.axis_index("lat") * rows
    col0 = lax.axis_index("lon") * cols + LANES
    mid = slice(LANES, 2 * LANES)
    clear_margins(s_ref, rows)

    def level(l, carry):
        for f in range(nf):
            for rt in range(tiles):
                x = [tile(x_ref, (f, l), rt * SUB, q, n, rem) for q in range(n)]
                for t in range(TAPS):
                    s_ref[f, t, SUB + rt * SUB : 2 * SUB + rt * SUB, :] = shifted(x[0], x[1], x[2], t)

        def step(rt, carry):
            at = pl.ds(pl.multiple_of(rt * SUB, SUB), SUB)
            kr = row_ref[l, at, mid] - (row0 + rt * SUB - HALO) - iota(0)
            kc = col_first(col_ref[l, at, mid], col0, total_cols)
            w = [w_ref[b, l, at, mid] for b in range(8)]

            def emit(f, v):
                o_ref[f, l, at, :] = v

            tile_loop(s_ref, lambda f: f, rt, kr, kc, w, nf, emit)
            return carry

        return lax.fori_loop(0, tiles, step, carry)

    lax.fori_loop(0, nl, level, 0)


def outer_kernel(
    x_ref, row_ref, col_ref, w_ref, west_ref, east_ref, o_ref, s_ref, *, rows, cols, rem, n, total_cols
):
    nf, nl = x_ref.shape[:2]
    tiles = rows // SUB
    row0 = lax.axis_index("lat") * rows
    col0 = lax.axis_index("lon") * cols
    clear_margins(s_ref, rows)

    def level(l, carry):
        west, east = west_ref[l], east_ref[l]
        for side, q in enumerate((0, n - 1)):
            for f in range(nf):
                for rt in range(tiles):
                    slot = f * tiles + rt
                    prev, nxt = None, None
                    if q:
                        prev = tile(x_ref, (f, l), rt * SUB, n - 2, n, rem)
                        cur = halo_tiles(west, east, slot, tile(x_ref, (f, l), rt * SUB, n - 1, n, rem), rem)[1]
                    else:
                        cur = tile(x_ref, (f, l), rt * SUB, 0, n, rem)
                        nxt = tile(x_ref, (f, l), rt * SUB, 1, n, rem)
                        prev = halo_tiles(west, east, slot, cur, rem)[0]
                    to = slice(SUB + rt * SUB, 2 * SUB + rt * SUB)
                    for t in range(TAPS):
                        s_ref[f, t, to, :] = shifted(prev, cur, nxt, t)

            def step(rt, carry):
                row = pl.multiple_of(rt * SUB, SUB)
                at = pl.ds(row, SUB)
                kr = tile(row_ref, (l,), row, q, n, rem) - (row0 + rt * SUB - HALO) - iota(0)
                kc = col_first(tile(col_ref, (l,), row, q, n, rem), col0 + q * LANES, total_cols)
                w = [tile(w_ref, (b, l), row, q, n, rem) for b in range(8)]

                def emit(f, v):
                    o_ref[f, l, at, side * LANES : (side + 1) * LANES] = v

                tile_loop(s_ref, lambda f: f, rt, kr, kc, w, nf, emit)
                return carry

            lax.fori_loop(0, tiles, step, 0)
        return carry

    lax.fori_loop(0, nl, level, 0)


def edge_kernel(
    cw_ref, ccw_ref, row_ref, col_ref, w_ref, mid_ref, out_ref, o_out, buf, sems,
    *, rows, cols, rem, n, half, total_cols
):
    nf, nl = cw_ref.shape[:2]
    row0 = lax.axis_index("lat") * rows
    col0 = lax.axis_index("lon") * cols
    upper = iota(0) < HALO
    low = jnp.full((SUB, LANES), lax.axis_index("lon"), jnp.int32) < half
    lane, sub = iota(1), iota(0)
    zero = jnp.zeros((SUB, LANES), jnp.float32)
    pad = jnp.zeros((SUB - HALO, LANES), jnp.float32)
    pick = lambda a, b: jnp.where(upper, a, b)
    down = rows - SUB

    def copy(l):
        return pltpu.make_async_copy(buf.at[:, l], o_out.at[:, l], sems.at[l])

    def level(l, carry):
        rc = []
        for q in range(n):
            both = lambda ref, lead: pick(tile(ref, lead, 0, q, n, rem), tile(ref, lead, down, q, n, rem))
            first = pick(sub + row0, sub + (row0 + down))
            kr = both(row_ref, (l,)) - first + HALO
            kc = col_first(both(col_ref, (l,)), col0 + q * LANES, total_cols)
            w = [both(w_ref, (b, l)) for b in range(8)]
            r = expand(kr, w[:4])
            rc.append(([pick(r[s], r[s + HALO]) for s in range(HALO)], expand(kc, w[4:])))
        for f in range(nf):
            v = []
            for q in range(n):
                lanes = slice(q * LANES, (q + 1) * LANES)
                a = jnp.concatenate([cw_ref[f, l, :, lanes], pad], axis=0)
                b = jnp.concatenate([ccw_ref[f, l, :, lanes], pad], axis=0)
                a, b = jnp.where(low, a, b), jnp.where(low, b, a)
                v.append([a] + [pltpu.roll(jnp.where(sub < s, b, a), SUB - s, 0) for s in range(1, HALO)])
            v.append([zero] * HALO)
            for q in range(n):
                r, c = rc[q]
                total = None
                for s in range(HALO):
                    line = None
                    for t in range(TAPS):
                        x = v[q][s]
                        if t:
                            x = pltpu.roll(jnp.where(lane < t, v[q + 1][s], x), LANES - t, 1)
                        line = c[t] * x if line is None else line + c[t] * x
                    line = r[s] * line
                    total = line if total is None else total + line
                width = min(LANES, cols - q * LANES)
                lanes = slice(q * LANES, q * LANES + width)
                for rt in range(rows // SUB):
                    at = slice(rt * SUB, rt * SUB + SUB)
                    if q == 1:
                        val = mid_ref[f, l, at, :]
                    else:
                        side = 1 if q else 0
                        val = out_ref[f, l, at, side * LANES : (side + 1) * LANES]
                    if rt == 0:
                        val = val + jnp.where(upper, total, 0.0)
                    if rt == rows // SUB - 1:
                        val = val + jnp.where(upper, 0.0, total)
                    buf[f, l, at, lanes] = val[:, :width]
        copy(l).start()
        return carry

    lax.fori_loop(0, nl, level, 0)
    for l in range(nl):
        copy(l).wait()


def circle(lat, lon):
    half = lon // 2
    pairs = []
    for s in range(lon):
        for b in range(lat):
            step = 1 if s < half else -1
            to = (b + step, s) if 0 <= b + step < lat else (b, (s + half) % lon)
            pairs.append((b * lon + s, to[0] * lon + to[1]))
    return pairs


def body(fields, dep_row, dep_col, weights):
    nf, nl, rows, cols = fields.shape
    lat, lon = lax.axis_size("lat"), lax.axis_size("lon")
    n = -(-cols // LANES)
    rem = cols - (n - 1) * LANES
    tiles = rows // SUB
    wide = n * LANES
    half = lon // 2
    total_cols = cols * lon
    assert n == 3 and HALO <= rem <= LANES - HALO and rows % SUB == 0
    f32 = jnp.float32
    shape = jax.ShapeDtypeStruct
    params = lambda: pltpu.CompilerParams(vmem_limit_bytes=VMEM)
    strip = shape((nl, SUB, LANES), f32)
    vmem = pl.BlockSpec(memory_space=pltpu.VMEM)
    hbm = pl.BlockSpec(memory_space=pl.ANY)

    west_out, east_out = pl.pallas_call(
        lambda *a: pack_kernel(*a, rem=rem, tiles=tiles, n=n),
        in_specs=[vmem],
        out_specs=[vmem] * 2,
        out_shape=[strip, strip],
        compiler_params=params(),
        name="pack",
    )(fields)
    up = [(i, (i + 1) % lon) for i in range(lon)]
    west = lax.ppermute(west_out, "lon", up)
    east = lax.ppermute(east_out, "lon", [(j, i) for i, j in up])

    mid = pl.pallas_call(
        lambda *a: inner_kernel(*a, rows=rows, cols=cols, rem=rem, n=n, total_cols=total_cols),
        in_specs=[vmem] * 4,
        out_specs=vmem,
        out_shape=shape((nf, nl, rows, LANES), f32),
        scratch_shapes=[pltpu.VMEM((nf, TAPS, rows + 2 * SUB, LANES), f32)],
        compiler_params=params(),
        name="inner",
    )(fields, dep_row, dep_col, weights)

    band_edge = shape((nf, nl, HALO, wide), f32)
    cw, ccw = pl.pallas_call(
        lambda *a: rowpack_kernel(*a, rem=rem, tiles=tiles, n=n, half=half),
        in_specs=[vmem] * 3 + [hbm],
        out_specs=[vmem] * 2,
        out_shape=[band_edge] * 2,
        compiler_params=params(),
        name="rowpack",
    )(fields, west, east, mid)
    ring = circle(lat, lon)
    cw = lax.ppermute(cw, ("lat", "lon"), ring)
    ccw = lax.ppermute(ccw, ("lat", "lon"), [(j, i) for i, j in ring])

    out = pl.pallas_call(
        lambda *a: outer_kernel(*a, rows=rows, cols=cols, rem=rem, n=n, total_cols=total_cols),
        in_specs=[vmem] * 6,
        out_specs=vmem,
        out_shape=shape((nf, nl, rows, 2 * LANES), f32),
        scratch_shapes=[pltpu.VMEM((nf, TAPS, rows + 2 * SUB, LANES), f32)],
        compiler_params=params(),
        name="outer",
    )(fields, dep_row, dep_col, weights, west, east)

    return pl.pallas_call(
        lambda *a: edge_kernel(*a, rows=rows, cols=cols, rem=rem, n=n, half=half, total_cols=total_cols),
        in_specs=[vmem] * 7,
        out_specs=hbm,
        out_shape=shape(fields.shape, f32),
        scratch_shapes=[pltpu.VMEM(fields.shape, f32), pltpu.SemaphoreType.DMA((nl,))],
        compiler_params=params(),
        name="edge",
    )(cw, ccw, dep_row, dep_col, weights, mid, out)


def solution(mesh):
    return jax.shard_map(
        body,
        mesh=mesh,
        in_specs=(
            P(None, None, "lat", "lon"),
            P(None, "lat", "lon"),
            P(None, "lat", "lon"),
            P(None, None, "lat", "lon"),
        ),
        out_specs=P(None, None, "lat", "lon"),
        check_vma=False,
    )
```

```python
import jax
import jax.numpy as jnp
from jax import lax
from jax.experimental import pallas as pl
from jax.experimental.pallas import tpu as pltpu
from jax.sharding import PartitionSpec as P

HALO = 4
TAPS = 2 * HALO
LANES = 128
SUB = 8
VMEM = 24 * 1024 * 1024


def iota(dim):
    return lax.broadcasted_iota(jnp.int32, (SUB, LANES), dim)


def tile(ref, lead, row, q, n, rem):
    at = pl.ds(row, SUB)
    if q < n - 1 or rem == LANES:
        return ref[(*lead, at, slice(q * LANES, (q + 1) * LANES))]
    part = ref[(*lead, at, slice(q * LANES, q * LANES + rem))]
    fill = jnp.zeros((SUB, LANES - rem), part.dtype)
    return jnp.concatenate([part, fill], axis=1)


def expand(k, w):
    masks = [k == v for v in range(HALO + 1)]
    out = []
    for t in range(TAPS):
        val = jnp.zeros((SUB, LANES), jnp.float32)
        for v in range(HALO + 1):
            if 0 <= t - v < 4:
                val = jnp.where(masks[v], w[t - v], val)
        out.append(val)
    return out


def shifted(prev, cur, nxt, t):
    lane = iota(1)
    if t < HALO:
        d = HALO - t
        return pltpu.roll(jnp.where(lane >= LANES - d, prev, cur), d, 1)
    if t == HALO:
        return cur
    e = t - HALO
    z = cur if nxt is None else jnp.where(lane < e, nxt, cur)
    return pltpu.roll(z, LANES - e, 1)


def col_first(dep, base, total_cols):
    off = dep - base - iota(1)
    return jnp.where(off > 0, off - total_cols, off) + HALO


def pack_kernel(x_ref, west_ref, east_ref, *, rem, tiles, n):
    lane = iota(1)
    nf, nl = x_ref.shape[:2]
    for l in range(nl):
        w = jnp.zeros((SUB, LANES), jnp.float32)
        e = jnp.zeros((SUB, LANES), jnp.float32)
        for f in range(nf):
            for rt in range(tiles):
                m = HALO * (f * tiles + rt)
                here = (lane >= m) & (lane < m + HALO)
                a = tile(x_ref, (f, l), rt * SUB, n - 1, n, rem)
                b = tile(x_ref, (f, l), rt * SUB, 0, n, rem)
                w = jnp.where(here, pltpu.roll(a, (m - (rem - HALO)) % LANES, 1), w)
                e = jnp.where(here, pltpu.roll(b, m, 1), e)
        west_ref[l] = w
        east_ref[l] = e


def halo_tiles(west, east, slot, last, rem):
    m = HALO * slot
    prev = pltpu.roll(west, (LANES - HALO - m) % LANES, 1)
    ends = jnp.where(iota(1) < rem, last, pltpu.roll(east, (rem - m) % LANES, 1))
    return prev, ends


def rowpack_kernel(x_ref, west_ref, east_ref, after, cw_ref, ccw_ref, *, rem, tiles, n, half):
    nf, nl, rows, _ = x_ref.shape
    band = lax.axis_index("lat")
    sector = lax.axis_index("lon")
    last_band = lax.axis_size("lat") - 1
    sub = iota(0)
    upper = sub < HALO
    full = lambda x: jnp.full((SUB, LANES), x, jnp.int32)
    flip = jnp.where(upper, full(band), last_band - full(band)) == 0
    low = full(sector) < half

    for l in range(nl):
        west, east = west_ref[l], east_ref[l]
        for f in range(nf):
            t = []
            for q in range(n):
                a = tile(x_ref, (f, l), 0, q, n, rem)
                b = tile(x_ref, (f, l), rows - SUB, q, n, rem)
                t.append(jnp.where(upper, a, b))
            slot_t, slot_b = f * tiles, f * tiles + tiles - 1
            pa, ea = halo_tiles(west, east, slot_t, t[-1], rem)
            pb, eb = halo_tiles(west, east, slot_b, t[-1], rem)
            prev = jnp.where(upper, pa, pb)
            t[-1] = jnp.where(upper, ea, eb)
            for q in range(n):
                v = shifted(t[q - 1] if q else prev, t[q], None, 0)
                r1 = sub % HALO
                rev = jnp.where(
                    r1 == 0,
                    pltpu.roll(v, SUB - 3, 0),
                    jnp.where(
                        r1 == 1,
                        pltpu.roll(v, SUB - 1, 0),
                        jnp.where(r1 == 2, pltpu.roll(v, 1, 0), pltpu.roll(v, 3, 0)),
                    ),
                )
                v = jnp.where(flip, rev, v)
                s = pltpu.roll(v, HALO, 0)
                cw_ref[f, l, :, q * LANES : (q + 1) * LANES] = jnp.where(low, s, v)[:HALO]
                ccw_ref[f, l, :, q * LANES : (q + 1) * LANES] = jnp.where(low, v, s)[:HALO]


def tile_loop(s_ref, rt, kr, kc, w, nf, emit, build):
    r = expand(kr, w[:4])
    c = expand(kc, w[4:])
    for f in range(nf):
        build(f)
        total = None
        for s in range(TAPS):
            line = None
            for t in range(TAPS):
                term = c[t] * s_ref[f, t, pl.ds(rt * SUB + HALO + s, SUB), :]
                line = term if line is None else line + term
            line = r[s] * line
            total = line if total is None else total + line
        emit(f, total)


def clear_margins(s_ref, rows):
    zero = jnp.zeros((SUB, LANES), jnp.float32)
    for i in range(s_ref.shape[0]):
        for t in range(TAPS):
            s_ref[i, t, 0:SUB, :] = zero
            s_ref[i, t, SUB + rows : 2 * SUB + rows, :] = zero


def inner_kernel(
    x_ref, row_ref, col_ref, w_hbm, o_ref, s0_ref, s1_ref, w_ref, sems, *, rows, cols, rem, n, total_cols
):
    nf, nl = x_ref.shape[:2]
    tiles = rows // SUB
    row0 = lax.axis_index("lat") * rows
    col0 = lax.axis_index("lon") * cols + LANES
    mid = slice(LANES, 2 * LANES)

    def fetch(l):
        return pltpu.make_async_copy(w_hbm.at[:, l, :, pl.ds(LANES, LANES)], w_ref.at[l], sems.at[l])

    for l in range(nl):
        fetch(l).start()
    clear_margins(s0_ref, rows)
    clear_margins(s1_ref, rows)

    def build(s_ref, l, rt, f):
        row = rt * SUB if isinstance(rt, int) else pl.multiple_of(rt * SUB, SUB)
        x = [tile(x_ref, (f, l), row, q, n, rem) for q in range(n)]
        for t in range(TAPS):
            s_ref[f, t, pl.ds(row + SUB, SUB), :] = shifted(x[0], x[1], x[2], t)

    for f in range(nf):
        for rt in range(tiles):
            build(s0_ref, 0, rt, f)

    def pair(p, carry):
        for side, (now, then) in enumerate(((s0_ref, s1_ref), (s1_ref, s0_ref))):
            l = 2 * p + side
            ahead = jnp.minimum(l + 1, nl - 1)
            fetch(l).wait()

            def step(rt, carry):
                at = pl.ds(pl.multiple_of(rt * SUB, SUB), SUB)
                kr = row_ref[l, at, mid] - (row0 + rt * SUB - HALO) - iota(0)
                kc = col_first(col_ref[l, at, mid], col0, total_cols)
                w = [w_ref[l, b, at, :] for b in range(8)]

                def emit(f, v):
                    o_ref[f, l, at, :] = v

                tile_loop(now, rt, kr, kc, w, nf, emit, lambda f: build(then, ahead, rt, f))
                return carry

            lax.fori_loop(0, tiles, step, 0)
        return carry

    lax.fori_loop(0, nl // 2, pair, 0)


def outer_kernel(
    x_ref, row_ref, col_ref, w_ref, west_ref, east_ref, o_ref, s0_ref, s1_ref, *, rows, cols, rem, n, total_cols
):
    nf, nl = x_ref.shape[:2]
    tiles = rows // SUB
    row0 = lax.axis_index("lat") * rows
    col0 = lax.axis_index("lon") * cols
    clear_margins(s0_ref, rows)
    clear_margins(s1_ref, rows)

    def build(s_ref, side, l, rt, f):
        row = rt * SUB if isinstance(rt, int) else pl.multiple_of(rt * SUB, SUB)
        m = HALO * (f * tiles + rt)
        if side:
            prev = tile(x_ref, (f, l), row, n - 2, n, rem)
            last = tile(x_ref, (f, l), row, n - 1, n, rem)
            cur = jnp.where(iota(1) < rem, last, pltpu.roll(east_ref[l], (rem + LANES - m) % LANES, 1))
            nxt = None
        else:
            prev = pltpu.roll(west_ref[l], (2 * LANES - HALO - m) % LANES, 1)
            cur = tile(x_ref, (f, l), row, 0, n, rem)
            nxt = tile(x_ref, (f, l), row, 1, n, rem)
        for t in range(TAPS):
            s_ref[f, t, pl.ds(row + SUB, SUB), :] = shifted(prev, cur, nxt, t)

    for f in range(nf):
        for rt in range(tiles):
            build(s0_ref, 0, 0, rt, f)

    def level(l, carry):
        for side, (now, then) in enumerate(((s0_ref, s1_ref), (s1_ref, s0_ref))):
            q = side * (n - 1)
            ahead = jnp.minimum(l + side, nl - 1)

            def step(rt, carry):
                row = pl.multiple_of(rt * SUB, SUB)
                at = pl.ds(row, SUB)
                kr = tile(row_ref, (l,), row, q, n, rem) - (row0 + rt * SUB - HALO) - iota(0)
                kc = col_first(tile(col_ref, (l,), row, q, n, rem), col0 + q * LANES, total_cols)
                w = [tile(w_ref, (b, l), row, q, n, rem) for b in range(8)]

                def emit(f, v):
                    o_ref[f, l, at, side * LANES : (side + 1) * LANES] = v

                tile_loop(now, rt, kr, kc, w, nf, emit, lambda f: build(then, 1 - side, ahead, rt, f))
                return carry

            lax.fori_loop(0, tiles, step, 0)
        return carry

    lax.fori_loop(0, nl, level, 0)


def edge_kernel(
    cw_ref, ccw_ref, row_ref, col_ref, w_ref, mid_ref, out_ref, o_out, buf, sems,
    *, rows, cols, rem, n, half, total_cols
):
    nf, nl = cw_ref.shape[:2]
    row0 = lax.axis_index("lat") * rows
    col0 = lax.axis_index("lon") * cols
    upper = iota(0) < HALO
    low = jnp.full((SUB, LANES), lax.axis_index("lon"), jnp.int32) < half
    lane, sub = iota(1), iota(0)
    zero = jnp.zeros((SUB, LANES), jnp.float32)
    pad = jnp.zeros((SUB - HALO, LANES), jnp.float32)
    pick = lambda a, b: jnp.where(upper, a, b)
    down = rows - SUB

    def copy(l):
        return pltpu.make_async_copy(buf.at[:, l], o_out.at[:, l], sems.at[l])

    def level(l, carry):
        rc = []
        for q in range(n):
            both = lambda ref, lead: pick(tile(ref, lead, 0, q, n, rem), tile(ref, lead, down, q, n, rem))
            first = pick(sub + row0, sub + (row0 + down))
            kr = both(row_ref, (l,)) - first + HALO
            kc = col_first(both(col_ref, (l,)), col0 + q * LANES, total_cols)
            w = [both(w_ref, (b, l)) for b in range(8)]
            r = expand(kr, w[:4])
            rc.append(([pick(r[s], r[s + HALO]) for s in range(HALO)], expand(kc, w[4:])))
        for f in range(nf):
            v = []
            for q in range(n):
                lanes = slice(q * LANES, (q + 1) * LANES)
                a = jnp.concatenate([cw_ref[f, l, :, lanes], pad], axis=0)
                b = jnp.concatenate([ccw_ref[f, l, :, lanes], pad], axis=0)
                a, b = jnp.where(low, a, b), jnp.where(low, b, a)
                v.append([a] + [pltpu.roll(jnp.where(sub < s, b, a), SUB - s, 0) for s in range(1, HALO)])
            v.append([zero] * HALO)
            for q in range(n):
                r, c = rc[q]
                total = None
                for s in range(HALO):
                    line = None
                    for t in range(TAPS):
                        x = v[q][s]
                        if t:
                            x = pltpu.roll(jnp.where(lane < t, v[q + 1][s], x), LANES - t, 1)
                        line = c[t] * x if line is None else line + c[t] * x
                    line = r[s] * line
                    total = line if total is None else total + line
                width = min(LANES, cols - q * LANES)
                lanes = slice(q * LANES, q * LANES + width)
                for rt in range(rows // SUB):
                    at = slice(rt * SUB, rt * SUB + SUB)
                    if q == 1:
                        val = mid_ref[f, l, at, :]
                    else:
                        side = 1 if q else 0
                        val = out_ref[f, l, at, side * LANES : (side + 1) * LANES]
                    if rt == 0:
                        val = val + jnp.where(upper, total, 0.0)
                    if rt == rows // SUB - 1:
                        val = val + jnp.where(upper, 0.0, total)
                    buf[f, l, at, lanes] = val[:, :width]
        copy(l).start()
        return carry

    lax.fori_loop(0, nl, level, 0)
    for l in range(nl):
        copy(l).wait()


def circle(lat, lon):
    half = lon // 2
    pairs = []
    for s in range(lon):
        for b in range(lat):
            step = 1 if s < half else -1
            to = (b + step, s) if 0 <= b + step < lat else (b, (s + half) % lon)
            pairs.append((b * lon + s, to[0] * lon + to[1]))
    return pairs


def body(fields, dep_row, dep_col, weights):
    nf, nl, rows, cols = fields.shape
    lat, lon = lax.axis_size("lat"), lax.axis_size("lon")
    n = -(-cols // LANES)
    rem = cols - (n - 1) * LANES
    tiles = rows // SUB
    wide = n * LANES
    half = lon // 2
    total_cols = cols * lon
    assert n == 3 and nl % 2 == 0 and HALO <= rem <= LANES - HALO and rows % SUB == 0
    f32 = jnp.float32
    shape = jax.ShapeDtypeStruct
    params = lambda: pltpu.CompilerParams(vmem_limit_bytes=VMEM)
    strip = shape((nl, SUB, LANES), f32)
    vmem = pl.BlockSpec(memory_space=pltpu.VMEM)
    hbm = pl.BlockSpec(memory_space=pl.ANY)

    west_out, east_out = pl.pallas_call(
        lambda *a: pack_kernel(*a, rem=rem, tiles=tiles, n=n),
        in_specs=[vmem],
        out_specs=[vmem] * 2,
        out_shape=[strip, strip],
        compiler_params=params(),
        name="pack",
    )(fields)
    up = [(i, (i + 1) % lon) for i in range(lon)]
    west = lax.ppermute(west_out, "lon", up)
    east = lax.ppermute(east_out, "lon", [(j, i) for i, j in up])

    shifts = pltpu.VMEM((nf, TAPS, rows + 2 * SUB, LANES), f32)
    mid = pl.pallas_call(
        lambda *a: inner_kernel(*a, rows=rows, cols=cols, rem=rem, n=n, total_cols=total_cols),
        in_specs=[vmem] * 3 + [pl.BlockSpec(memory_space=pltpu.HBM)],
        out_specs=vmem,
        out_shape=shape((nf, nl, rows, LANES), f32),
        scratch_shapes=[shifts, shifts, pltpu.VMEM((nl, 8, rows, LANES), f32), pltpu.SemaphoreType.DMA((nl,))],
        compiler_params=params(),
        name="inner",
    )(fields, dep_row, dep_col, weights)

    band_edge = shape((nf, nl, HALO, wide), f32)
    cw, ccw = pl.pallas_call(
        lambda *a: rowpack_kernel(*a, rem=rem, tiles=tiles, n=n, half=half),
        in_specs=[vmem] * 3 + [hbm],
        out_specs=[vmem] * 2,
        out_shape=[band_edge] * 2,
        compiler_params=params(),
        name="rowpack",
    )(fields, west, east, mid)
    ring = circle(lat, lon)
    cw = lax.ppermute(cw, ("lat", "lon"), ring)
    ccw = lax.ppermute(ccw, ("lat", "lon"), [(j, i) for i, j in ring])

    out = pl.pallas_call(
        lambda *a: outer_kernel(*a, rows=rows, cols=cols, rem=rem, n=n, total_cols=total_cols),
        in_specs=[vmem] * 6,
        out_specs=vmem,
        out_shape=shape((nf, nl, rows, 2 * LANES), f32),
        scratch_shapes=[shifts, shifts],
        compiler_params=params(),
        name="outer",
    )(fields, dep_row, dep_col, weights, west, east)

    return pl.pallas_call(
        lambda *a: edge_kernel(*a, rows=rows, cols=cols, rem=rem, n=n, half=half, total_cols=total_cols),
        in_specs=[vmem] * 7,
        out_specs=hbm,
        out_shape=shape(fields.shape, f32),
        scratch_shapes=[pltpu.VMEM(fields.shape, f32), pltpu.SemaphoreType.DMA((nl,))],
        compiler_params=params(),
        name="edge",
    )(cw, ccw, dep_row, dep_col, weights, mid, out)


def solution(mesh):
    return jax.shard_map(
        body,
        mesh=mesh,
        in_specs=(
            P(None, None, "lat", "lon"),
            P(None, "lat", "lon"),
            P(None, "lat", "lon"),
            P(None, None, "lat", "lon"),
        ),
        out_specs=P(None, None, "lat", "lon"),
        check_vma=False,
    )
```

```python
import jax
import jax.numpy as jnp
from jax import lax
from jax.experimental import pallas as pl
from jax.experimental.pallas import tpu as pltpu
from jax.sharding import PartitionSpec as P

HALO = 4
TAPS = 2 * HALO
LANES = 128
SUB = 8
VMEM = 24 * 1024 * 1024


def iota(dim):
    return lax.broadcasted_iota(jnp.int32, (SUB, LANES), dim)


def tile(ref, lead, row, q, n, rem):
    at = pl.ds(row, SUB)
    if q < n - 1 or rem == LANES:
        return ref[(*lead, at, slice(q * LANES, (q + 1) * LANES))]
    part = ref[(*lead, at, slice(q * LANES, q * LANES + rem))]
    fill = jnp.zeros((SUB, LANES - rem), part.dtype)
    return jnp.concatenate([part, fill], axis=1)


def expand(k, w):
    masks = [k == v for v in range(HALO + 1)]
    out = []
    for t in range(TAPS):
        val = jnp.zeros((SUB, LANES), jnp.float32)
        for v in range(HALO + 1):
            if 0 <= t - v < 4:
                val = jnp.where(masks[v], w[t - v], val)
        out.append(val)
    return out


def shifted(prev, cur, nxt, t):
    lane = iota(1)
    if t < HALO:
        d = HALO - t
        return pltpu.roll(jnp.where(lane >= LANES - d, prev, cur), d, 1)
    if t == HALO:
        return cur
    e = t - HALO
    z = cur if nxt is None else jnp.where(lane < e, nxt, cur)
    return pltpu.roll(z, LANES - e, 1)


def col_first(dep, base, total_cols):
    off = dep - base - iota(1)
    return jnp.where(off > 0, off - total_cols, off) + HALO


def pack_kernel(x_ref, west_ref, east_ref, *, rem, tiles, n):
    lane = iota(1)
    nf, nl = x_ref.shape[:2]
    for l in range(nl):
        w = jnp.zeros((SUB, LANES), jnp.float32)
        e = jnp.zeros((SUB, LANES), jnp.float32)
        for f in range(nf):
            for rt in range(tiles):
                m = HALO * (f * tiles + rt)
                here = (lane >= m) & (lane < m + HALO)
                a = tile(x_ref, (f, l), rt * SUB, n - 1, n, rem)
                b = tile(x_ref, (f, l), rt * SUB, 0, n, rem)
                w = jnp.where(here, pltpu.roll(a, (m - (rem - HALO)) % LANES, 1), w)
                e = jnp.where(here, pltpu.roll(b, m, 1), e)
        west_ref[l] = w
        east_ref[l] = e


def halo_tiles(west, east, slot, last, rem):
    m = HALO * slot
    prev = pltpu.roll(west, (LANES - HALO - m) % LANES, 1)
    ends = jnp.where(iota(1) < rem, last, pltpu.roll(east, (rem - m) % LANES, 1))
    return prev, ends


def rowpack_kernel(x_ref, west_ref, east_ref, after, cw_ref, ccw_ref, *, rem, tiles, n, half):
    nf, nl, rows, _ = x_ref.shape
    band = lax.axis_index("lat")
    sector = lax.axis_index("lon")
    last_band = lax.axis_size("lat") - 1
    sub = iota(0)
    upper = sub < HALO
    full = lambda x: jnp.full((SUB, LANES), x, jnp.int32)
    flip = jnp.where(upper, full(band), last_band - full(band)) == 0
    low = full(sector) < half

    for l in range(nl):
        west, east = west_ref[l], east_ref[l]
        for f in range(nf):
            t = []
            for q in range(n):
                a = tile(x_ref, (f, l), 0, q, n, rem)
                b = tile(x_ref, (f, l), rows - SUB, q, n, rem)
                t.append(jnp.where(upper, a, b))
            slot_t, slot_b = f * tiles, f * tiles + tiles - 1
            pa, ea = halo_tiles(west, east, slot_t, t[-1], rem)
            pb, eb = halo_tiles(west, east, slot_b, t[-1], rem)
            prev = jnp.where(upper, pa, pb)
            t[-1] = jnp.where(upper, ea, eb)
            for q in range(n):
                v = shifted(t[q - 1] if q else prev, t[q], None, 0)
                r1 = sub % HALO
                rev = jnp.where(
                    r1 == 0,
                    pltpu.roll(v, SUB - 3, 0),
                    jnp.where(
                        r1 == 1,
                        pltpu.roll(v, SUB - 1, 0),
                        jnp.where(r1 == 2, pltpu.roll(v, 1, 0), pltpu.roll(v, 3, 0)),
                    ),
                )
                v = jnp.where(flip, rev, v)
                s = pltpu.roll(v, HALO, 0)
                cw_ref[f, l, :, q * LANES : (q + 1) * LANES] = jnp.where(low, s, v)[:HALO]
                ccw_ref[f, l, :, q * LANES : (q + 1) * LANES] = jnp.where(low, v, s)[:HALO]


def tile_loop(s_ref, base, rt, kr, kc, w, nf, emit):
    r = expand(kr, w[:4])
    c = expand(kc, w[4:])
    for f in range(nf):
        total = None
        for s in range(TAPS):
            line = None
            for t in range(TAPS):
                term = c[t] * s_ref[base(f), t, pl.ds(rt * SUB + HALO + s, SUB), :]
                line = term if line is None else line + term
            line = r[s] * line
            total = line if total is None else total + line
        emit(f, total)


def clear_margins(s_ref, rows):
    zero = jnp.zeros((SUB, LANES), jnp.float32)
    for i in range(s_ref.shape[0]):
        for t in range(TAPS):
            s_ref[i, t, 0:SUB, :] = zero
            s_ref[i, t, SUB + rows : 2 * SUB + rows, :] = zero


def inner_kernel(x_ref, row_ref, col_ref, w_ref, o_ref, s_ref, *, rows, cols, rem, n, total_cols):
    nf, nl = x_ref.shape[:2]
    tiles = rows // SUB
    row0 = lax.axis_index("lat") * rows
    col0 = lax.axis_index("lon") * cols + LANES
    mid = slice(LANES, 2 * LANES)
    clear_margins(s_ref, rows)

    def level(l, carry):
        for f in range(nf):
            for rt in range(tiles):
                x = [tile(x_ref, (f, l), rt * SUB, q, n, rem) for q in range(n)]
                for t in range(TAPS):
                    s_ref[f, t, SUB + rt * SUB : 2 * SUB + rt * SUB, :] = shifted(x[0], x[1], x[2], t)

        def step(rt, carry):
            at = pl.ds(pl.multiple_of(rt * SUB, SUB), SUB)
            kr = row_ref[l, at, mid] - (row0 + rt * SUB - HALO) - iota(0)
            kc = col_first(col_ref[l, at, mid], col0, total_cols)
            w = [w_ref[b, l, at, mid] for b in range(8)]

            def emit(f, v):
                o_ref[f, l, at, :] = v

            tile_loop(s_ref, lambda f: f, rt, kr, kc, w, nf, emit)
            return carry

        return lax.fori_loop(0, tiles, step, carry)

    lax.fori_loop(0, nl, level, 0)


def outer_kernel(
    x_ref, row_ref, col_ref, w_ref, west_ref, east_ref, o_ref, s_ref, *, rows, cols, rem, n, total_cols
):
    nf, nl = x_ref.shape[:2]
    tiles = rows // SUB
    row0 = lax.axis_index("lat") * rows
    col0 = lax.axis_index("lon") * cols
    clear_margins(s_ref, rows)

    def level(l, carry):
        west, east = west_ref[l], east_ref[l]
        for side, q in enumerate((0, n - 1)):
            for f in range(nf):
                for rt in range(tiles):
                    slot = f * tiles + rt
                    prev, nxt = None, None
                    if q:
                        prev = tile(x_ref, (f, l), rt * SUB, n - 2, n, rem)
                        cur = halo_tiles(west, east, slot, tile(x_ref, (f, l), rt * SUB, n - 1, n, rem), rem)[1]
                    else:
                        cur = tile(x_ref, (f, l), rt * SUB, 0, n, rem)
                        nxt = tile(x_ref, (f, l), rt * SUB, 1, n, rem)
                        prev = halo_tiles(west, east, slot, cur, rem)[0]
                    to = slice(SUB + rt * SUB, 2 * SUB + rt * SUB)
                    for t in range(TAPS):
                        s_ref[f, t, to, :] = shifted(prev, cur, nxt, t)

            def step(rt, carry):
                row = pl.multiple_of(rt * SUB, SUB)
                at = pl.ds(row, SUB)
                kr = tile(row_ref, (l,), row, q, n, rem) - (row0 + rt * SUB - HALO) - iota(0)
                kc = col_first(tile(col_ref, (l,), row, q, n, rem), col0 + q * LANES, total_cols)
                w = [tile(w_ref, (b, l), row, q, n, rem) for b in range(8)]

                def emit(f, v):
                    o_ref[f, l, at, side * LANES : (side + 1) * LANES] = v

                tile_loop(s_ref, lambda f: f, rt, kr, kc, w, nf, emit)
                return carry

            lax.fori_loop(0, tiles, step, 0)
        return carry

    lax.fori_loop(0, nl, level, 0)


def edge_kernel(
    cw_ref, ccw_ref, row_ref, col_ref, w_ref, mid_ref, out_ref, o_out, buf, sems,
    *, rows, cols, rem, n, half, total_cols
):
    nf, nl = cw_ref.shape[:2]
    row0 = lax.axis_index("lat") * rows
    col0 = lax.axis_index("lon") * cols
    upper = iota(0) < HALO
    low = jnp.full((SUB, LANES), lax.axis_index("lon"), jnp.int32) < half
    lane, sub = iota(1), iota(0)
    zero = jnp.zeros((SUB, LANES), jnp.float32)
    pad = jnp.zeros((SUB - HALO, LANES), jnp.float32)
    pick = lambda a, b: jnp.where(upper, a, b)
    down = rows - SUB

    def copy(l):
        return pltpu.make_async_copy(buf.at[:, l], o_out.at[:, l], sems.at[l])

    def level(l, carry):
        rc = []
        for q in range(n):
            both = lambda ref, lead: pick(tile(ref, lead, 0, q, n, rem), tile(ref, lead, down, q, n, rem))
            first = pick(sub + row0, sub + (row0 + down))
            kr = both(row_ref, (l,)) - first + HALO
            kc = col_first(both(col_ref, (l,)), col0 + q * LANES, total_cols)
            w = [both(w_ref, (b, l)) for b in range(8)]
            r = expand(kr, w[:4])
            rc.append(([pick(r[s], r[s + HALO]) for s in range(HALO)], expand(kc, w[4:])))
        for f in range(nf):
            v = []
            for q in range(n):
                lanes = slice(q * LANES, (q + 1) * LANES)
                a = jnp.concatenate([cw_ref[f, l, :, lanes], pad], axis=0)
                b = jnp.concatenate([ccw_ref[f, l, :, lanes], pad], axis=0)
                a, b = jnp.where(low, a, b), jnp.where(low, b, a)
                v.append([a] + [pltpu.roll(jnp.where(sub < s, b, a), SUB - s, 0) for s in range(1, HALO)])
            v.append([zero] * HALO)
            for q in range(n):
                r, c = rc[q]
                total = None
                for s in range(HALO):
                    line = None
                    for t in range(TAPS):
                        x = v[q][s]
                        if t:
                            x = pltpu.roll(jnp.where(lane < t, v[q + 1][s], x), LANES - t, 1)
                        line = c[t] * x if line is None else line + c[t] * x
                    line = r[s] * line
                    total = line if total is None else total + line
                width = min(LANES, cols - q * LANES)
                lanes = slice(q * LANES, q * LANES + width)
                for rt in range(rows // SUB):
                    at = slice(rt * SUB, rt * SUB + SUB)
                    if q == 1:
                        val = mid_ref[f, l, at, :]
                    else:
                        side = 1 if q else 0
                        val = out_ref[f, l, at, side * LANES : (side + 1) * LANES]
                    if rt == 0:
                        val = val + jnp.where(upper, total, 0.0)
                    if rt == rows // SUB - 1:
                        val = val + jnp.where(upper, 0.0, total)
                    buf[f, l, at, lanes] = val[:, :width]
        copy(l).start()
        return carry

    lax.fori_loop(0, nl, level, 0)
    for l in range(nl):
        copy(l).wait()


def circle(lat, lon):
    half = lon // 2
    pairs = []
    for s in range(lon):
        for b in range(lat):
            step = 1 if s < half else -1
            to = (b + step, s) if 0 <= b + step < lat else (b, (s + half) % lon)
            pairs.append((b * lon + s, to[0] * lon + to[1]))
    return pairs


def body(fields, dep_row, dep_col, weights):
    nf, nl, rows, cols = fields.shape
    lat, lon = lax.axis_size("lat"), lax.axis_size("lon")
    n = -(-cols // LANES)
    rem = cols - (n - 1) * LANES
    tiles = rows // SUB
    wide = n * LANES
    half = lon // 2
    total_cols = cols * lon
    assert n == 3 and HALO <= rem <= LANES - HALO and rows % SUB == 0
    f32 = jnp.float32
    shape = jax.ShapeDtypeStruct
    params = lambda: pltpu.CompilerParams(vmem_limit_bytes=VMEM)
    strip = shape((nl, SUB, LANES), f32)
    vmem = pl.BlockSpec(memory_space=pltpu.VMEM)
    hbm = pl.BlockSpec(memory_space=pl.ANY)

    west_out, east_out = pl.pallas_call(
        lambda *a: pack_kernel(*a, rem=rem, tiles=tiles, n=n),
        in_specs=[vmem],
        out_specs=[vmem] * 2,
        out_shape=[strip, strip],
        compiler_params=params(),
        name="pack",
    )(fields)
    up = [(i, (i + 1) % lon) for i in range(lon)]
    west = lax.ppermute(west_out, "lon", up)
    east = lax.ppermute(east_out, "lon", [(j, i) for i, j in up])

    mid = pl.pallas_call(
        lambda *a: inner_kernel(*a, rows=rows, cols=cols, rem=rem, n=n, total_cols=total_cols),
        in_specs=[vmem] * 4,
        out_specs=vmem,
        out_shape=shape((nf, nl, rows, LANES), f32),
        scratch_shapes=[pltpu.VMEM((nf, TAPS, rows + 3 * SUB, LANES), f32)],
        compiler_params=params(),
        name="inner",
    )(fields, dep_row, dep_col, weights)

    band_edge = shape((nf, nl, HALO, wide), f32)
    cw, ccw = pl.pallas_call(
        lambda *a: rowpack_kernel(*a, rem=rem, tiles=tiles, n=n, half=half),
        in_specs=[vmem] * 3 + [hbm],
        out_specs=[vmem] * 2,
        out_shape=[band_edge] * 2,
        compiler_params=params(),
        name="rowpack",
    )(fields, west, east, mid)
    ring = circle(lat, lon)
    cw = lax.ppermute(cw, ("lat", "lon"), ring)
    ccw = lax.ppermute(ccw, ("lat", "lon"), [(j, i) for i, j in ring])

    out = pl.pallas_call(
        lambda *a: outer_kernel(*a, rows=rows, cols=cols, rem=rem, n=n, total_cols=total_cols),
        in_specs=[vmem] * 6,
        out_specs=vmem,
        out_shape=shape((nf, nl, rows, 2 * LANES), f32),
        scratch_shapes=[pltpu.VMEM((nf, TAPS, rows + 3 * SUB, LANES), f32)],
        compiler_params=params(),
        name="outer",
    )(fields, dep_row, dep_col, weights, west, east)

    return pl.pallas_call(
        lambda *a: edge_kernel(*a, rows=rows, cols=cols, rem=rem, n=n, half=half, total_cols=total_cols),
        in_specs=[vmem] * 7,
        out_specs=hbm,
        out_shape=shape(fields.shape, f32),
        scratch_shapes=[pltpu.VMEM(fields.shape, f32), pltpu.SemaphoreType.DMA((nl,))],
        compiler_params=params(),
        name="edge",
    )(cw, ccw, dep_row, dep_col, weights, mid, out)


def solution(mesh):
    return jax.shard_map(
        body,
        mesh=mesh,
        in_specs=(
            P(None, None, "lat", "lon"),
            P(None, "lat", "lon"),
            P(None, "lat", "lon"),
            P(None, None, "lat", "lon"),
        ),
        out_specs=P(None, None, "lat", "lon"),
        check_vma=False,
    )
```

```python
import jax
import jax.numpy as jnp
from jax import lax
from jax.experimental import pallas as pl
from jax.experimental.pallas import tpu as pltpu
from jax.sharding import PartitionSpec as P

HALO = 4
TAPS = 2 * HALO
LANES = 128
SUB = 8
VMEM = 24 * 1024 * 1024


def iota(dim):
    return lax.broadcasted_iota(jnp.int32, (SUB, LANES), dim)


def tile(ref, lead, row, q, n, rem):
    at = pl.ds(row, SUB)
    if q < n - 1 or rem == LANES:
        return ref[(*lead, at, slice(q * LANES, (q + 1) * LANES))]
    part = ref[(*lead, at, slice(q * LANES, q * LANES + rem))]
    fill = jnp.zeros((SUB, LANES - rem), part.dtype)
    return jnp.concatenate([part, fill], axis=1)


def expand(k, w):
    masks = [k == v for v in range(HALO + 1)]
    out = []
    for t in range(TAPS):
        val = jnp.zeros((SUB, LANES), jnp.float32)
        for v in range(HALO + 1):
            if 0 <= t - v < 4:
                val = jnp.where(masks[v], w[t - v], val)
        out.append(val)
    return out


def shifted(prev, cur, nxt, t):
    lane = iota(1)
    if t < HALO:
        d = HALO - t
        return pltpu.roll(jnp.where(lane >= LANES - d, prev, cur), d, 1)
    if t == HALO:
        return cur
    e = t - HALO
    z = cur if nxt is None else jnp.where(lane < e, nxt, cur)
    return pltpu.roll(z, LANES - e, 1)


def col_first(dep, base, total_cols):
    off = dep - base - iota(1)
    return jnp.where(off > 0, off - total_cols, off) + HALO


def pack_kernel(x_ref, west_ref, east_ref, *, rem, tiles, n):
    lane = iota(1)
    nf, nl = x_ref.shape[:2]
    for l in range(nl):
        w = jnp.zeros((SUB, LANES), jnp.float32)
        e = jnp.zeros((SUB, LANES), jnp.float32)
        for f in range(nf):
            for rt in range(tiles):
                m = HALO * (f * tiles + rt)
                here = (lane >= m) & (lane < m + HALO)
                a = tile(x_ref, (f, l), rt * SUB, n - 1, n, rem)
                b = tile(x_ref, (f, l), rt * SUB, 0, n, rem)
                w = jnp.where(here, pltpu.roll(a, (m - (rem - HALO)) % LANES, 1), w)
                e = jnp.where(here, pltpu.roll(b, m, 1), e)
        west_ref[l] = w
        east_ref[l] = e


def halo_tiles(west, east, slot, last, rem):
    m = HALO * slot
    prev = pltpu.roll(west, (LANES - HALO - m) % LANES, 1)
    ends = jnp.where(iota(1) < rem, last, pltpu.roll(east, (rem - m) % LANES, 1))
    return prev, ends


def rowpack_kernel(x_ref, west_ref, east_ref, after, cw_ref, ccw_ref, *, rem, tiles, n, half):
    nf, nl, rows, _ = x_ref.shape
    band = lax.axis_index("lat")
    sector = lax.axis_index("lon")
    last_band = lax.axis_size("lat") - 1
    sub = iota(0)
    upper = sub < HALO
    full = lambda x: jnp.full((SUB, LANES), x, jnp.int32)
    flip = jnp.where(upper, full(band), last_band - full(band)) == 0
    low = full(sector) < half

    for l in range(nl):
        west, east = west_ref[l], east_ref[l]
        for f in range(nf):
            t = []
            for q in range(n):
                a = tile(x_ref, (f, l), 0, q, n, rem)
                b = tile(x_ref, (f, l), rows - SUB, q, n, rem)
                t.append(jnp.where(upper, a, b))
            slot_t, slot_b = f * tiles, f * tiles + tiles - 1
            pa, ea = halo_tiles(west, east, slot_t, t[-1], rem)
            pb, eb = halo_tiles(west, east, slot_b, t[-1], rem)
            prev = jnp.where(upper, pa, pb)
            t[-1] = jnp.where(upper, ea, eb)
            for q in range(n):
                v = shifted(t[q - 1] if q else prev, t[q], None, 0)
                r1 = sub % HALO
                rev = jnp.where(
                    r1 == 0,
                    pltpu.roll(v, SUB - 3, 0),
                    jnp.where(
                        r1 == 1,
                        pltpu.roll(v, SUB - 1, 0),
                        jnp.where(r1 == 2, pltpu.roll(v, 1, 0), pltpu.roll(v, 3, 0)),
                    ),
                )
                v = jnp.where(flip, rev, v)
                s = pltpu.roll(v, HALO, 0)
                cw_ref[f, l, :, q * LANES : (q + 1) * LANES] = jnp.where(low, s, v)[:HALO]
                ccw_ref[f, l, :, q * LANES : (q + 1) * LANES] = jnp.where(low, v, s)[:HALO]


def tile_loop(s_ref, base, rt, kr, kc, w, nf, emit):
    r = expand(kr, w[:4])
    c = expand(kc, w[4:])
    for f in range(nf):
        total = None
        for s in range(TAPS):
            line = None
            for t in range(TAPS):
                term = c[t] * s_ref[base(f), t, pl.ds(rt * SUB + HALO + s, SUB), :]
                line = term if line is None else line + term
            line = r[s] * line
            total = line if total is None else total + line
        emit(f, total)


def clear_margins(s_ref, rows):
    zero = jnp.zeros((SUB, LANES), jnp.float32)
    for i in range(s_ref.shape[0]):
        for t in range(TAPS):
            s_ref[i, t, 0:SUB, :] = zero
            s_ref[i, t, SUB + rows : 2 * SUB + rows, :] = zero


def inner_kernel(x_ref, row_ref, col_ref, w_ref, o_ref, s_ref, *, rows, cols, rem, n, total_cols):
    nf, nl = x_ref.shape[:2]
    tiles = rows // SUB
    row0 = lax.axis_index("lat") * rows
    col0 = lax.axis_index("lon") * cols + LANES
    mid = slice(LANES, 2 * LANES)
    clear_margins(s_ref, rows)

    def level(l, carry):
        for f in range(nf):
            for rt in range(tiles):
                x = [tile(x_ref, (f, l), rt * SUB, q, n, rem) for q in range(n)]
                for t in range(TAPS):
                    s_ref[f, t, SUB + rt * SUB : 2 * SUB + rt * SUB, :] = shifted(x[0], x[1], x[2], t)

        def step(rt, carry):
            at = pl.ds(pl.multiple_of(rt * SUB, SUB), SUB)
            kr = row_ref[l, at, mid] - (row0 + rt * SUB - HALO) - iota(0)
            kc = col_first(col_ref[l, at, mid], col0, total_cols)
            w = [w_ref[b, l, at, mid] for b in range(8)]

            def emit(f, v):
                o_ref[f, l, at, :] = v

            tile_loop(s_ref, lambda f: f, rt, kr, kc, w, nf, emit)
            return carry

        return lax.fori_loop(0, tiles, step, carry, unroll=2)

    lax.fori_loop(0, nl, level, 0)


def outer_kernel(
    x_ref, row_ref, col_ref, w_ref, west_ref, east_ref, o_ref, s_ref, *, rows, cols, rem, n, total_cols
):
    nf, nl = x_ref.shape[:2]
    tiles = rows // SUB
    row0 = lax.axis_index("lat") * rows
    col0 = lax.axis_index("lon") * cols
    clear_margins(s_ref, rows)

    def level(l, carry):
        west, east = west_ref[l], east_ref[l]
        for side, q in enumerate((0, n - 1)):
            for f in range(nf):
                for rt in range(tiles):
                    slot = f * tiles + rt
                    prev, nxt = None, None
                    if q:
                        prev = tile(x_ref, (f, l), rt * SUB, n - 2, n, rem)
                        cur = halo_tiles(west, east, slot, tile(x_ref, (f, l), rt * SUB, n - 1, n, rem), rem)[1]
                    else:
                        cur = tile(x_ref, (f, l), rt * SUB, 0, n, rem)
                        nxt = tile(x_ref, (f, l), rt * SUB, 1, n, rem)
                        prev = halo_tiles(west, east, slot, cur, rem)[0]
                    to = slice(SUB + rt * SUB, 2 * SUB + rt * SUB)
                    for t in range(TAPS):
                        s_ref[f, t, to, :] = shifted(prev, cur, nxt, t)

            def step(rt, carry):
                row = pl.multiple_of(rt * SUB, SUB)
                at = pl.ds(row, SUB)
                kr = tile(row_ref, (l,), row, q, n, rem) - (row0 + rt * SUB - HALO) - iota(0)
                kc = col_first(tile(col_ref, (l,), row, q, n, rem), col0 + q * LANES, total_cols)
                w = [tile(w_ref, (b, l), row, q, n, rem) for b in range(8)]

                def emit(f, v):
                    o_ref[f, l, at, side * LANES : (side + 1) * LANES] = v

                tile_loop(s_ref, lambda f: f, rt, kr, kc, w, nf, emit)
                return carry

            lax.fori_loop(0, tiles, step, 0, unroll=2)
        return carry

    lax.fori_loop(0, nl, level, 0)


def edge_kernel(
    cw_ref, ccw_ref, row_ref, col_ref, w_ref, mid_ref, out_ref, o_out, buf, sems,
    *, rows, cols, rem, n, half, total_cols
):
    nf, nl = cw_ref.shape[:2]
    row0 = lax.axis_index("lat") * rows
    col0 = lax.axis_index("lon") * cols
    upper = iota(0) < HALO
    low = jnp.full((SUB, LANES), lax.axis_index("lon"), jnp.int32) < half
    lane, sub = iota(1), iota(0)
    zero = jnp.zeros((SUB, LANES), jnp.float32)
    pad = jnp.zeros((SUB - HALO, LANES), jnp.float32)
    pick = lambda a, b: jnp.where(upper, a, b)
    down = rows - SUB

    def copy(l):
        return pltpu.make_async_copy(buf.at[:, l], o_out.at[:, l], sems.at[l])

    def level(l, carry):
        rc = []
        for q in range(n):
            both = lambda ref, lead: pick(tile(ref, lead, 0, q, n, rem), tile(ref, lead, down, q, n, rem))
            first = pick(sub + row0, sub + (row0 + down))
            kr = both(row_ref, (l,)) - first + HALO
            kc = col_first(both(col_ref, (l,)), col0 + q * LANES, total_cols)
            w = [both(w_ref, (b, l)) for b in range(8)]
            r = expand(kr, w[:4])
            rc.append(([pick(r[s], r[s + HALO]) for s in range(HALO)], expand(kc, w[4:])))
        for f in range(nf):
            v = []
            for q in range(n):
                lanes = slice(q * LANES, (q + 1) * LANES)
                a = jnp.concatenate([cw_ref[f, l, :, lanes], pad], axis=0)
                b = jnp.concatenate([ccw_ref[f, l, :, lanes], pad], axis=0)
                a, b = jnp.where(low, a, b), jnp.where(low, b, a)
                v.append([a] + [pltpu.roll(jnp.where(sub < s, b, a), SUB - s, 0) for s in range(1, HALO)])
            v.append([zero] * HALO)
            for q in range(n):
                r, c = rc[q]
                total = None
                for s in range(HALO):
                    line = None
                    for t in range(TAPS):
                        x = v[q][s]
                        if t:
                            x = pltpu.roll(jnp.where(lane < t, v[q + 1][s], x), LANES - t, 1)
                        line = c[t] * x if line is None else line + c[t] * x
                    line = r[s] * line
                    total = line if total is None else total + line
                width = min(LANES, cols - q * LANES)
                lanes = slice(q * LANES, q * LANES + width)
                for rt in range(rows // SUB):
                    at = slice(rt * SUB, rt * SUB + SUB)
                    if q == 1:
                        val = mid_ref[f, l, at, :]
                    else:
                        side = 1 if q else 0
                        val = out_ref[f, l, at, side * LANES : (side + 1) * LANES]
                    if rt == 0:
                        val = val + jnp.where(upper, total, 0.0)
                    if rt == rows // SUB - 1:
                        val = val + jnp.where(upper, 0.0, total)
                    buf[f, l, at, lanes] = val[:, :width]
        copy(l).start()
        return carry

    lax.fori_loop(0, nl, level, 0)
    for l in range(nl):
        copy(l).wait()


def circle(lat, lon):
    half = lon // 2
    pairs = []
    for s in range(lon):
        for b in range(lat):
            step = 1 if s < half else -1
            to = (b + step, s) if 0 <= b + step < lat else (b, (s + half) % lon)
            pairs.append((b * lon + s, to[0] * lon + to[1]))
    return pairs


def body(fields, dep_row, dep_col, weights):
    nf, nl, rows, cols = fields.shape
    lat, lon = lax.axis_size("lat"), lax.axis_size("lon")
    n = -(-cols // LANES)
    rem = cols - (n - 1) * LANES
    tiles = rows // SUB
    wide = n * LANES
    half = lon // 2
    total_cols = cols * lon
    assert n == 3 and HALO <= rem <= LANES - HALO and rows % SUB == 0
    f32 = jnp.float32
    shape = jax.ShapeDtypeStruct
    params = lambda: pltpu.CompilerParams(vmem_limit_bytes=VMEM)
    strip = shape((nl, SUB, LANES), f32)
    vmem = pl.BlockSpec(memory_space=pltpu.VMEM)
    hbm = pl.BlockSpec(memory_space=pl.ANY)

    west_out, east_out = pl.pallas_call(
        lambda *a: pack_kernel(*a, rem=rem, tiles=tiles, n=n),
        in_specs=[vmem],
        out_specs=[vmem] * 2,
        out_shape=[strip, strip],
        compiler_params=params(),
        name="pack",
    )(fields)
    up = [(i, (i + 1) % lon) for i in range(lon)]
    west = lax.ppermute(west_out, "lon", up)
    east = lax.ppermute(east_out, "lon", [(j, i) for i, j in up])

    mid = pl.pallas_call(
        lambda *a: inner_kernel(*a, rows=rows, cols=cols, rem=rem, n=n, total_cols=total_cols),
        in_specs=[vmem] * 4,
        out_specs=vmem,
        out_shape=shape((nf, nl, rows, LANES), f32),
        scratch_shapes=[pltpu.VMEM((nf, TAPS, rows + 3 * SUB, LANES), f32)],
        compiler_params=params(),
        name="inner",
    )(fields, dep_row, dep_col, weights)

    band_edge = shape((nf, nl, HALO, wide), f32)
    cw, ccw = pl.pallas_call(
        lambda *a: rowpack_kernel(*a, rem=rem, tiles=tiles, n=n, half=half),
        in_specs=[vmem] * 3 + [hbm],
        out_specs=[vmem] * 2,
        out_shape=[band_edge] * 2,
        compiler_params=params(),
        name="rowpack",
    )(fields, west, east, mid)
    ring = circle(lat, lon)
    cw = lax.ppermute(cw, ("lat", "lon"), ring)
    ccw = lax.ppermute(ccw, ("lat", "lon"), [(j, i) for i, j in ring])

    out = pl.pallas_call(
        lambda *a: outer_kernel(*a, rows=rows, cols=cols, rem=rem, n=n, total_cols=total_cols),
        in_specs=[vmem] * 6,
        out_specs=vmem,
        out_shape=shape((nf, nl, rows, 2 * LANES), f32),
        scratch_shapes=[pltpu.VMEM((nf, TAPS, rows + 3 * SUB, LANES), f32)],
        compiler_params=params(),
        name="outer",
    )(fields, dep_row, dep_col, weights, west, east)

    return pl.pallas_call(
        lambda *a: edge_kernel(*a, rows=rows, cols=cols, rem=rem, n=n, half=half, total_cols=total_cols),
        in_specs=[vmem] * 7,
        out_specs=hbm,
        out_shape=shape(fields.shape, f32),
        scratch_shapes=[pltpu.VMEM(fields.shape, f32), pltpu.SemaphoreType.DMA((nl,))],
        compiler_params=params(),
        name="edge",
    )(cw, ccw, dep_row, dep_col, weights, mid, out)


def solution(mesh):
    return jax.shard_map(
        body,
        mesh=mesh,
        in_specs=(
            P(None, None, "lat", "lon"),
            P(None, "lat", "lon"),
            P(None, "lat", "lon"),
            P(None, None, "lat", "lon"),
        ),
        out_specs=P(None, None, "lat", "lon"),
        check_vma=False,
    )
```
